32 devices in a mesh: rep: 1 (over z), dp: 32 (over x, y, core).
Axes of the slice: x: 4, y: 4, z: 1, core: 2. Of those that a mesh axis runs over, the one named last changes fastest.
The devices are a block of a 4x4x8 slice.
Arguments:
- x: bfloat16 [32, 2048, 512], P(('rep', 'dp'))
- dy: bfloat16 [32, 2048, 512], P(('rep', 'dp'))
- wq: bfloat16 [2, 512, 512], replicated
- wk: bfloat16 [2, 512, 256], replicated
- wv: bfloat16 [2, 512, 256], replicated
- wo: bfloat16 [2, 512, 512], replicated
- w_gate: bfloat16 [2, 512, 1536], replicated
- w_up: bfloat16 [2, 512, 1536], replicated
- w_down: bfloat16 [2, 1536, 512], replicated
- m_wq: float32 [2, 512, 512], replicated
- m_wk: float32 [2, 512, 256], replicated
- m_wv: float32 [2, 512, 256], replicated
- m_wo: float32 [2, 512, 512], replicated
- m_w_gate: float32 [2, 512, 1536], replicated
- m_w_up: float32 [2, 512, 1536], replicated
- m_w_down: float32 [2, 1536, 512], replicated
- v_wq: float32 [2, 512, 512], replicated
- v_wk: float32 [2, 512, 256], replicated
- v_wv: float32 [2, 512, 256], replicated
- v_wo: float32 [2, 512, 512], replicated
- v_w_gate: float32 [2, 512, 1536], replicated
- v_w_up: float32 [2, 512, 1536], replicated
- v_w_down: float32 [2, 1536, 512], replicated
Outputs:
- output 1: bfloat16 [2, 512, 512], P('rep')
- output 2: bfloat16 [2, 512, 256], P('rep')
- output 3: bfloat16 [2, 512, 256], P('rep')
- output 4: bfloat16 [2, 512, 512], P('rep')
- output 5: bfloat16 [2, 512, 1536], P('rep')
- output 6: bfloat16 [2, 512, 1536], P('rep')
- output 7: bfloat16 [2, 1536, 512], P('rep')
- output 8: float32 [2, 512, 512], P('rep')
- output 9: float32 [2, 512, 256], P('rep')
- output 10: float32 [2, 512, 256], P('rep')
- output 11: float32 [2, 512, 512], P('rep')
- output 12: float32 [2, 512, 1536], P('rep')
- output 13: float32 [2, 512, 1536], P('rep')
- output 14: float32 [2, 1536, 512], P('rep')
- output 15: float32 [2, 512, 512], P('rep')
- output 16: float32 [2, 512, 256], P('rep')
- output 17: float32 [2, 512, 256], P('rep')
- output 18: float32 [2, 512, 512], P('rep')
- output 19: float32 [2, 512, 1536], P('rep')
- output 20: float32 [2, 512, 1536], P('rep')
- output 21: float32 [2, 1536, 512], P('rep')
All inputs are finite; a program needn't handle non-finite values.
Results may differ from the reference program's by a relative error of at most 0.0247.
Values are sent between devices in bfloat16 or wider.
A program may use at most 768 MiB of HBM per device.

```python
import jax
import jax.numpy as jnp
from jax import lax

SEQUENCES = 32
TOKENS = 2048
D = 512
HEADS = 4
KV_HEADS = 2
HEAD = 128
FF = 1536
LAYERS = 2
THETA = 10000
NAMES = ("wq", "wk", "wv", "wo", "w_gate", "w_up", "w_down")
SHAPES = {
    "wq": (LAYERS, D, HEADS * HEAD),
    "wk": (LAYERS, D, KV_HEADS * HEAD),
    "wv": (LAYERS, D, KV_HEADS * HEAD),
    "wo": (LAYERS, HEADS * HEAD, D),
    "w_gate": (LAYERS, D, FF),
    "w_up": (LAYERS, D, FF),
    "w_down": (LAYERS, FF, D),
}


def bump(key, n, height):
    away = (jnp.arange(n, dtype=jnp.int32) - jax.random.randint(key, (), 0, n, jnp.int32)) % n
    return jnp.where(away < n // 8, height, 1.0)


def together(key, own, strength):
    shared = jax.random.normal(key, own.shape[1:], jnp.float32)
    return (own + strength * shared) * lax.rsqrt(1 + strength * strength)


def setup_inputs(seed: int = 0, part: int = 0) -> dict:
    kx, kdy, ka, kb, kz, kf, kh, kl, *keys = jax.random.split(jax.random.key(seed), 8 + 3 * len(NAMES))
    kx, kdy, ka, kb = (jax.random.fold_in(k, part) for k in (kx, kdy, ka, kb))
    kw, km, kv = (keys[i::3] for i in range(3))
    shape = (SEQUENCES, TOKENS, D)
    much_x, much_dy = jax.random.uniform(kz, (2,), jnp.float32, 0.0, 1.0)
    loud = 2.0 ** jax.random.uniform(jax.random.fold_in(kz, 1), (), jnp.float32, -1.0, 2.0)
    layers = 2.0 ** jax.random.uniform(kl, (LAYERS, 1, 1), jnp.float32, -1.0, 1.0)
    times = {"wq": 1.0, "wk": 1.0, "wv": 2.0, "wo": layers, "w_gate": 1.0, "w_up": bump(kh, FF, 4.0), "w_down": layers}
    x = together(ka, jax.random.normal(kx, shape, jnp.float32), much_x) * bump(kf, D, 4.0)
    dy = together(kb, jax.random.normal(kdy, shape, jnp.float32), much_dy)
    drawn = {"x": x.astype(jnp.bfloat16), "dy": (loud * dy * (SEQUENCES * TOKENS) ** -0.5).astype(jnp.bfloat16)}
    for key, name in zip(kw, NAMES, strict=True):
        drawn[name] = (jax.random.normal(key, SHAPES[name], jnp.float32) * SHAPES[name][1] ** -0.5 * times[name]).astype(jnp.bfloat16)
    for key, name in zip(km, NAMES, strict=True):
        drawn[f"m_{name}"] = 0.1 * jax.random.normal(key, SHAPES[name], jnp.float32)
    for key, name in zip(kv, NAMES, strict=True):
        drawn[f"v_{name}"] = jax.random.uniform(key, SHAPES[name], jnp.float32, 0.02, 0.06)
    return drawn


def matmul(a, w):
    return jnp.dot(a, w, preferred_element_type=jnp.float32).astype(jnp.bfloat16)


def normed(h):
    wide = h.astype(jnp.float32)
    scale = lax.rsqrt(jnp.mean(wide**2, -1, keepdims=True) + 1e-6)
    return (wide * scale).astype(jnp.bfloat16)


def turned(t, theta):
    half = t.shape[-1] // 2
    angle = jnp.arange(t.shape[0], dtype=jnp.float32)[:, None] * theta ** (-jnp.arange(half, dtype=jnp.float32) / half)
    cos, sin = jnp.cos(angle)[:, None], jnp.sin(angle)[:, None]
    a, b = t[..., :half].astype(jnp.float32), t[..., half:].astype(jnp.float32)
    return jnp.concatenate([a * cos - b * sin, b * cos + a * sin], -1).astype(jnp.bfloat16)


def seen_by(q, k, v):
    tokens, kv = q.shape[0], k.shape[1]
    q = q.reshape(tokens, kv, -1, q.shape[-1])
    scores = jnp.einsum("tgsd,ugd->gstu", q.astype(jnp.float32), k.astype(jnp.float32)) * q.shape[-1] ** -0.5
    place = jnp.arange(tokens)
    weights = jax.nn.softmax(jnp.where(place[:, None] >= place, scores, -jnp.inf), -1).astype(jnp.bfloat16)
    return jnp.einsum("gstu,ugd->tgsd", weights.astype(jnp.float32), v.astype(jnp.float32)).astype(jnp.bfloat16).reshape(tokens, -1)


def layer(h, w):
    a = normed(h)
    q, k = (turned(matmul(a, w[name]).reshape(h.shape[0], -1, HEAD), THETA) for name in ("wq", "wk"))
    h = h + matmul(seen_by(q, k, matmul(a, w["wv"]).reshape(h.shape[0], -1, HEAD)), w["wo"])
    b = normed(h)
    gate = jnp.dot(b, w["w_gate"], preferred_element_type=jnp.float32)
    up = jnp.dot(b, w["w_up"], preferred_element_type=jnp.float32)
    return h + matmul((jax.nn.silu(gate) * up).astype(jnp.bfloat16), w["w_down"])


def adamw(w, m, v, g):
    m = 0.9 * m + 0.1 * g
    v = 0.95 * v + 0.05 * g * g
    step = m * lax.rsqrt(v + 1e-8) + 0.1 * w
    return (w - 0.02 * step).astype(jnp.bfloat16), m, v


def clipped(gradients, sum_of_squares, count):
    factor = jnp.minimum(1.0, 0.5 * lax.rsqrt(sum_of_squares / count + 1e-30))
    return [g * factor for g in gradients]


def stack(weights, h):
    return lax.scan(lambda h, w: (layer(h, w), None), h, weights)[0]


def reference(x, dy, wq, wk, wv, wo, w_gate, w_up, w_down, m_wq, m_wk, m_wv, m_wo, m_w_gate, m_w_up, m_w_down, v_wq, v_wk, v_wv, v_wo, v_w_gate, v_w_up, v_w_down):
    weights = dict(zip(NAMES, (wq, wk, wv, wo, w_gate, w_up, w_down), strict=True))

    def take(so_far, sequence):
        h, by_y = sequence
        _, back = jax.vjp(stack, weights, h)
        by_weights, by_h = back(by_y)
        return jax.tree.map(lambda total, term: total + term.astype(jnp.float32), so_far, by_weights), by_h

    none_yet = {name: jnp.zeros(w.shape, jnp.float32) for name, w in weights.items()}
    by_weights, by_x = lax.scan(take, none_yet, (x, dy))
    gradients = [by_weights[name].astype(jnp.bfloat16).astype(jnp.float32) for name in NAMES]
    gradients = clipped(gradients, sum(jnp.sum(g * g) for g in gradients), sum(g.size for g in gradients))
    first = (m_wq, m_wk, m_wv, m_wo, m_w_gate, m_w_up, m_w_down)
    second = (v_wq, v_wk, v_wv, v_wo, v_w_gate, v_w_up, v_w_down)
    new = [adamw(weights[name].astype(jnp.float32), m, v, g) for name, m, v, g in zip(NAMES, first, second, gradients, strict=True)]
    return tuple(one[which] for which in range(3) for one in new)
```

```python
import functools
import math

import jax
import jax.numpy as jnp
from jax import lax
from jax.experimental import pallas as pl
from jax.experimental.pallas import tpu as pltpu
from jax.sharding import PartitionSpec as P

HEAD = 128
THETA = 10000
NAMES = ("wq", "wk", "wv", "wo", "w_gate", "w_up", "w_down")
NEG = -1e30
HIDDEN = 2 * NEG
LOG2E = 1.4426950408889634
VMEM = 66060288
F32, BF16 = jnp.float32, jnp.bfloat16

ROWS = 512
CHUNK, TALK_CHUNK = 1536, 512
QUERIES = 1024
KEYS, BACK_KEYS = 512, 256
STEP = 512


def fit(size, want, unit=128):
    return max(n for n in range(unit, max(min(want, size), unit) + 1, unit) if size % n == 0)


def dot(a, b, turned=False):
    return lax.dot_general(a, b, (((1,), (int(turned),)), ((), ())), preferred_element_type=F32)


def scale_of(wide):
    return lax.rsqrt(jnp.mean(wide * wide, -1, keepdims=True) + 1e-6)


def norm_back(wide, scale, by):
    return scale * (by - wide * (scale * scale * jnp.mean(by * wide, -1, keepdims=True)))


def turn(t, cos, sin):
    return t * cos + pltpu.roll(t, HEAD // 2, 1) * sin


def unturn(t, cos, sin):
    return t * cos - pltpu.roll(t, HEAD // 2, 1) * sin


def params(*semantics, talks=None):
    more = {} if talks is None else {"collective_id": talks, "has_side_effects": True}
    return pltpu.CompilerParams(dimension_semantics=semantics, vmem_limit_bytes=VMEM, **more)


ANY = pl.BlockSpec(memory_space=pl.ANY)


def at(slot, when, *actions):
    @pl.when(slot == when)
    def _():
        for action in actions:
            action()


def whole(shape):
    return pl.BlockSpec(shape, lambda *_: (0,) * len(shape))


def of_layer(w, number):
    return pl.BlockSpec((None, *w.shape[1:]), lambda *_: (number, 0, 0), pipeline_mode=pl.Buffered(1))


def rows_of(width, rows):
    return pl.BlockSpec((rows, width), lambda i: (i, 0))


TALK = (2, 2, 6, 4)
UNIT = 16


def places(n):
    side = math.isqrt(n // 2)
    me = lax.axis_index("dp")
    core, y, x = lax.rem(me, 2), lax.rem(lax.div(me, 2), side), lax.div(me, 2 * side)
    at = lambda x, y: (x * side + y) * 2 + core
    near = lambda a: a + 1 - 2 * lax.rem(a, 2)
    bit = lambda a: lax.rem(lax.div(a + 1, 2), 2)
    return [(me + 1 - 2 * core, core), (at(near(x), y), bit(x)), (at(x, near(y)), bit(y)),
            (at(side - 1 - x, y), lax.div(x, 2)), (at(x, side - 1 - y), lax.div(y, 2))]


class GroupSum:
    def __init__(self, grads, out, units, lands, sems, n, compact=False):
        self.grads, self.out, self.lands, self.sems = grads, out, lands, sems
        spots = places(n)
        self.partner = [device for device, _ in spots]
        half = units // 2
        self.half, self.mine, self.other = half, spots[0][1] * half, (1 - spots[0][1]) * half
        land, offs, size = half, [self.mine + q * (half // 4) for q in range(4)], half // 4
        self.steps = [None]
        for k in range(4):
            size //= 2
            now = []
            for q in range(4):
                dim = 1 + (q + k) % 4
                bit = spots[dim][1]
                now.append((self.partner[dim], offs[q] + (1 - bit) * size, offs[q] + bit * size, size, land))
                offs[q] = offs[q] + bit * size
                land += size
            self.steps.append(now)
        first = [kept for _, _, kept, _, _ in self.steps[3]]
        self.moved = (lambda q, where: q * 2 * size + where - first[q]) if compact else (lambda q, where: where)

    def remote(self, src, dst, row, q, device, out):
        return pltpu.make_async_remote_copy(src, dst, self.sems.at[int(out), 0, row, q], self.sems.at[int(out), 1, row, q],
                                            device_id={"dp": device}, device_id_type=pl.DeviceIdType.MESH)

    def across(self, part, out):
        made = []
        for q, step in enumerate(self.steps[1]):
            where, size = step[1 + part], step[3]
            if out:
                src = dst = self.out.at[pl.ds(where, size)]
            else:
                src, dst = self.grads.at[pl.ds(where - self.mine + self.other, size)], self.lands.at[pl.ds(where - self.mine, size)]
            made.append(self.remote(src, dst, 5 * part, q, self.partner[0], out))
        return made

    def along(self, k, out):
        made = []
        for q, (device, sent, kept, size, land) in enumerate(self.steps[k]):
            if out:
                src = dst = self.out.at[pl.ds(self.moved(q, kept), size)]
            else:
                src, dst = self.grads.at[pl.ds(sent, size)], self.lands.at[pl.ds(land, size)]
            made.append(self.remote(src, dst, k, q, device, out))
        return made

    def add(self, to, where, land, size, into=None):
        many = math.gcd(size, 12)
        into = where if into is None else into

        def step(i, _):
            total = self.grads[pl.ds(where + i * many, many)].astype(F32) + self.lands[pl.ds(land + i * many, many)].astype(F32)
            to[pl.ds(into + i * many, many)] = total.astype(BF16)

        lax.fori_loop(0, size // many, step, None)

    def halve(self, k):
        if k == 0:
            start(self.across(0, False) + self.across(1, False))
        elif k == 1:
            wait(self.across(0, False))
            for _, sent, kept, size, _ in self.steps[1]:
                self.add(self.grads, sent, sent - self.mine, size)
            start(self.along(1, False))
            wait(self.across(1, False))
            for _, sent, kept, size, _ in self.steps[1]:
                self.add(self.grads, kept, kept - self.mine, size)
        else:
            wait(self.along(k - 1, False))
            for part in (1, 2):
                for now, (_, _, before, _, land) in zip(self.steps[k], self.steps[k - 1]):
                    self.add(self.grads, now[part], land + now[part] - before, now[3])
                if part == 1:
                    start(self.along(k, False))

    def turn(self):
        wait(self.along(4, False))
        for q, (_, _, kept, size, land) in enumerate(self.steps[4]):
            self.add(self.out, kept, land, size, self.moved(q, kept))
        start(self.along(4, True))

    def double(self, k, begin=False):
        if not begin:
            wait(self.along(k + 1, True))
        start(self.along(k, True) if k else self.across(0, True))
        if k == 1:
            start(self.across(1, True))

    def end(self):
        wait(self.across(0, True) + self.across(1, True))

    def after(self, k):
        return [(kept, size) for _, _, kept, size, _ in self.steps[k]]


def start(copies):
    for copy in copies:
        copy.start()


def wait(copies):
    for copy in copies:
        copy.wait()


def landing(units):
    return units - units // 32


def local_copies(pairs, sems, first=0):
    return [pltpu.make_async_copy(src, dst, sems.at[first + i]) for i, (src, dst) in enumerate(pairs)]


def greet(partners):
    barrier = pltpu.get_barrier_semaphore()
    for device in partners:
        pl.semaphore_signal(barrier, inc=1, device_id={"dp": device}, device_id_type=pl.DeviceIdType.MESH)
    pl.semaphore_wait(barrier, len(partners))


def _project(h_ref, wq_ref, wk_ref, wv_ref, cos_ref, sin_ref, q_ref, k_ref, v_ref):
    wide = h_ref[...].astype(F32)
    a = (wide * scale_of(wide)).astype(BF16)
    cos, sin = cos_ref[...], sin_ref[...]
    for w_ref, o_ref in ((wq_ref, q_ref), (wk_ref, k_ref)):
        t = dot(a, w_ref[...]).astype(BF16).astype(F32)
        for at in range(0, t.shape[1], HEAD):
            o_ref[:, at : at + HEAD] = turn(t[:, at : at + HEAD], cos, sin).astype(BF16)
    v_ref[...] = dot(a, wv_ref[...]).astype(BF16)


def project(h, wq, wk, wv, cos, sin, number):
    t, d = h.shape
    rows = fit(t, ROWS)
    dq, dk = wq.shape[2], wk.shape[2]
    return pl.pallas_call(
        _project,
        grid=(t // rows,),
        in_specs=[rows_of(d, rows), of_layer(wq, number), of_layer(wk, number), of_layer(wv, number), rows_of(HEAD, rows), rows_of(HEAD, rows)],
        out_specs=[rows_of(dq, rows), rows_of(dk, rows), rows_of(dk, rows)],
        out_shape=[jax.ShapeDtypeStruct((t, n), BF16) for n in (dq, dk, dk)],
        compiler_params=params("arbitrary"),
        name="project",
    )(h, wq, wk, wv, cos, sin)


def _diagonal(bq, bk, wide):
    out = []
    for m in range(-(-bq // bk)):
        out.append((m, {r: m * bk + bk - 1 > r for r in range(0, bq, wide) if m * bk < r + wide}))
    return out


def _attend(q_ref, k_ref, v_ref, o_ref, lse_ref, top_s, mix_s, *, scale, bq, bk, wide, kv, g):
    iq = pl.program_id(0)
    e = scale * LOG2E
    pieces = [(p, i, i * g + n, r) for p, (i, n, r) in
              enumerate((i, n, r) for i in range(kv) for n in range(g) for r in range(0, bq, wide))]
    top_s[...] = jnp.full(top_s.shape, NEG, F32)
    mix_s[...] = jnp.zeros(mix_s.shape, F32)
    ones = jnp.ones((8, bk), BF16)
    gap = lax.broadcasted_iota(jnp.int32, (bk, wide), 1) - lax.broadcasted_iota(jnp.int32, (bk, wide), 0)

    def block(j, strips, m=0):
        here = pl.ds(pl.multiple_of(j * bk, bk), bk)
        now = [x for x in pieces if strips is None or x[3] in strips]
        scores = [dot(k_ref[here, i * HEAD : (i + 1) * HEAD], q_ref[r : r + wide, h * HEAD : (h + 1) * HEAD], True) for _, i, h, r in now]
        weights, keeps = [], []
        for (p, i, h, r), s in zip(now, scores):
            if strips is not None and strips[r]:
                s = jnp.where(gap >= m * bk - r, s, HIDDEN)
            old = top_s[p : p + 1, :]
            top = jnp.maximum(old, s.max(axis=0, keepdims=True))
            top_s[p : p + 1, :] = top
            weights.append(jnp.exp2((s - top) * e).astype(BF16))
            keeps.append(jnp.exp2((old - top) * e))
        values = [jnp.concatenate([v_ref[here, i * HEAD : (i + 1) * HEAD].T, ones], axis=0) for i in range(kv)]
        for (p, i, h, r), w, keep in zip(now, weights, keeps):
            mix_s[p] = mix_s[p] * keep + dot(values[i], w)

    first = lax.div(iq * bq, bk)
    lax.fori_loop(0, first, lambda j, _: block(j, None), None)
    for m, strips in _diagonal(bq, bk, wide):
        block(first + m, strips, m)
    for p, i, h, r in pieces:
        total = mix_s[p, HEAD : HEAD + 1, :]
        o_ref[r : r + wide, h * HEAD : (h + 1) * HEAD] = (mix_s[p, :HEAD, :] * (1 / total)).T.astype(BF16)
        lse_ref[h : h + 1, r : r + wide] = top_s[p : p + 1, :] * scale + jnp.log(total)


def attend(q, k, v):
    t = q.shape[0]
    heads, kv = q.shape[1] // HEAD, k.shape[1] // HEAD
    bq = fit(t, QUERIES)
    bk = wide = fit(bq, KEYS)
    n = heads * (bq // wide)
    return pl.pallas_call(
        functools.partial(_attend, scale=HEAD**-0.5, bq=bq, bk=bk, wide=wide, kv=kv, g=heads // kv),
        grid=(t // bq,),
        in_specs=[rows_of(q.shape[1], bq), whole(k.shape), whole(v.shape)],
        out_specs=[rows_of(q.shape[1], bq), pl.BlockSpec((heads, bq), lambda i: (0, i))],
        out_shape=[jax.ShapeDtypeStruct(q.shape, BF16), jax.ShapeDtypeStruct((heads, t), F32)],
        scratch_shapes=[pltpu.VMEM((n, wide), F32), pltpu.VMEM((n, HEAD + 8, wide), F32)],
        compiler_params=params("arbitrary"),
        name="attend",
    )(q, k, v)


def _attend_back(q_ref, k_ref, v_ref, do_ref, lse_ref, delta_ref, *refs, scale, bq, bk, wide, kv, g, n):
    iq = pl.program_id(0)
    if n:
        part_ref, dq_ref, dk_ref, dv_ref, sum_ref, dq_s, dk_s, dv_s, sum_s, sems, local = refs
        work = GroupSum(None, sum_s, sum_s.shape[0], None, sems, n)
        takes = local_copies([(part_ref.at[pl.ds(q * size, size)], sum_s.at[pl.ds(first, size)]) for q, (first, size) in enumerate(work.after(3))], local)
        gives = local_copies([(sum_s.at[pl.ds(first, work.half)], sum_ref.at[pl.ds(first, work.half)]) for first in (work.mine, work.other)], local, 4)
    else:
        dq_ref, dk_ref, dv_ref, dq_s, dk_s, dv_s = refs

    e = scale * LOG2E
    pieces = [(i, i * g + n, r) for i in range(kv) for n in range(g) for r in range(0, bq, wide)]

    @pl.when(iq == 0)
    def _():
        dk_s[...] = jnp.zeros_like(dk_s)
        dv_s[...] = jnp.zeros_like(dv_s)

    dq_s[...] = jnp.zeros_like(dq_s)
    gap = lax.broadcasted_iota(jnp.int32, (bk, wide), 1) - lax.broadcasted_iota(jnp.int32, (bk, wide), 0)

    def block(j, strips, m=0):
        here = pl.ds(pl.multiple_of(j * bk, bk), bk)
        now = [x for x in pieces if strips is None or x[2] in strips]
        col = lambda n: slice(n * HEAD, (n + 1) * HEAD)
        qs = [q_ref[r : r + wide, col(h)] for _, h, r in now]
        dos = [do_ref[r : r + wide, col(h)] for _, h, r in now]
        scores = [dot(k_ref[here, col(i)], x, True) for (i, _, _), x in zip(now, qs)]
        dps = [dot(v_ref[here, col(i)], x, True) for (i, _, _), x in zip(now, dos)]
        turned = [k_ref[here, col(i)].T for i in range(kv)]
        for (i, h, r), q, do, s, dp in zip(now, qs, dos, scores, dps):
            p = jnp.exp2(s * e - lse_ref[h : h + 1, r : r + wide] * LOG2E)
            if strips is not None and strips[r]:
                p = jnp.where(gap >= m * bk - r, p, 0.0)
            ds = (p * (dp - delta_ref[h : h + 1, r : r + wide])).astype(BF16)
            dv_s[i, here, :] += dot(p.astype(BF16), do)
            dk_s[i, here, :] += dot(ds, q)
            dq_s[h, :, r : r + wide] += dot(turned[i], ds)

    first = lax.div(iq * bq, bk)
    last = pl.num_programs(0) - 1

    def loop(j, _):
        if n:
            at(iq * bq + j, last * bq + 1, lambda: work.double(1))
        block(j, None)

    if n:
        at(iq, 0, lambda: start(takes), lambda: greet(work.partner), lambda: wait(takes), lambda: work.double(3, True))
    lax.fori_loop(0, first, loop, None)
    for m, strips in _diagonal(bq, bk, wide):
        if n and m == 1:
            at(iq, last, lambda: work.double(0), lambda: gives[0].start())
        if n and m == 2:
            at(iq, 0, lambda: work.double(2))
        block(first + m, strips, m)
    for h in range(kv * g):
        dq_ref[:, h * HEAD : (h + 1) * HEAD] = (dq_s[h] * scale).T.astype(BF16)

    @pl.when(iq == last)
    def _():
        for i in range(kv):
            dk_ref[:, i * HEAD : (i + 1) * HEAD] = (dk_s[i] * scale).astype(BF16)
            dv_ref[:, i * HEAD : (i + 1) * HEAD] = dv_s[i].astype(BF16)
        if n:
            work.end()
            gives[1].start()
            wait(gives)


def attend_back(q, k, v, do, lse, delta, part=None, units=0, n=0):
    t = q.shape[0]
    heads, kv = q.shape[1] // HEAD, k.shape[1] // HEAD
    bq = fit(t, QUERIES)
    bk = wide = fit(bq, BACK_KEYS)
    stats = pl.BlockSpec((heads, bq), lambda i: (0, i))
    return pl.pallas_call(
        functools.partial(_attend_back, scale=HEAD**-0.5, bq=bq, bk=bk, wide=wide, kv=kv, g=heads // kv, n=n),
        grid=(t // bq,),
        in_specs=[rows_of(q.shape[1], bq), whole(k.shape), whole(v.shape), rows_of(q.shape[1], bq), stats, stats] + [ANY] * bool(n),
        out_specs=[rows_of(q.shape[1], bq), whole(k.shape), whole(v.shape)] + [ANY] * bool(n),
        out_shape=[jax.ShapeDtypeStruct(x.shape, BF16) for x in (q, k, v)] + ([jax.ShapeDtypeStruct((units, *part.shape[1:]), BF16)] if n else []),
        scratch_shapes=[pltpu.VMEM((heads, HEAD, bq), F32), pltpu.VMEM((kv, t, HEAD), F32), pltpu.VMEM((kv, t, HEAD), F32)]
        + ([pltpu.VMEM((units, *part.shape[1:]), BF16), pltpu.SemaphoreType.DMA(TALK), pltpu.SemaphoreType.DMA((6,))] if n else []),
        compiler_params=params("arbitrary", talks=2 if n else None),
        name="attend_back",
    )(q, k, v, do, lse, delta, *([part] if n else []))


def _mlp(h_ref, o_ref, wo_ref, wg_ref, wu_ref, wd_ref, mid_ref, out_ref, acc_s, *, chunk):
    mid = h_ref[...] + dot(o_ref[...], wo_ref[...]).astype(BF16)
    mid_ref[...] = mid
    wide = mid.astype(F32)
    b = (wide * scale_of(wide)).astype(BF16)
    acc_s[...] = jnp.zeros_like(acc_s)

    def step(c, _):
        here = pl.ds(pl.multiple_of(c * chunk, chunk), chunk)
        gate, up = dot(b, wg_ref[:, here]), dot(b, wu_ref[:, here])
        acc_s[...] += dot((gate * jax.nn.sigmoid(gate) * up).astype(BF16), wd_ref[here, :])

    lax.fori_loop(0, wg_ref.shape[1] // chunk, step, None)
    out_ref[...] = mid + acc_s[...].astype(BF16)


def mlp(h, o, wo, wg, wu, wd, number):
    t, d = h.shape
    rows = fit(t, ROWS)
    ff = wg.shape[2]
    return pl.pallas_call(
        functools.partial(_mlp, chunk=fit(ff, CHUNK)),
        grid=(t // rows,),
        in_specs=[rows_of(d, rows), rows_of(o.shape[1], rows)] + [of_layer(w, number) for w in (wo, wg, wu, wd)],
        out_specs=[rows_of(d, rows)] * 2,
        out_shape=[jax.ShapeDtypeStruct((t, d), BF16)] * 2,
        scratch_shapes=[pltpu.VMEM((rows, d), F32)],
        compiler_params=params("arbitrary"),
        name="mlp",
    )(h, o, wo, wg, wu, wd)


def _mlp_back(*refs, chunk, last, n, sizes):
    if n:
        (*ins, early_ref, late_ref), outs, scratch = refs[:9], refs[9:14], refs[14:]
        (*outs, part_ref), (*scratch, sum_s, part_s, lands, sems, local) = outs, scratch
        refs = (*ins, *outs, *scratch)
    (h_ref, dy_ref, o_ref, wo_ref, wg_ref, wu_ref, wd_ref,
     dmid_ref, do_ref, delta_ref, grads_ref, db_s, dwo_s, dwg_s, dwu_s, dwd_s) = refs
    step_of = pl.program_id(0)

    @pl.when(step_of == 0)
    def _():
        for s in (dwo_s, dwg_s, dwu_s, dwd_s):
            s[...] = jnp.zeros_like(s)

    if n:
        work = GroupSum(sum_s, part_s, sum(sizes), lands, sems, n, compact=True)
        loads = local_copies([(early_ref, sum_s.at[pl.ds(0, sizes[0])]), (late_ref, sum_s.at[pl.ds(*sizes)])], local)
        give = pltpu.make_async_copy(part_s, part_ref, local.at[2])

    def talk(c):
        if not n:
            return
        chunks = wg_ref.shape[1] // chunk
        slot, slots = step_of * chunks + c, pl.num_programs(0) * chunks
        on = lambda when, *actions: at(slot, lax.div(when * slots, 12), *actions)
        on(0, lambda: start(loads), lambda: greet(work.partner))
        on(1, lambda: wait(loads), lambda: work.halve(0))
        on(3, lambda: work.halve(1))
        on(6, lambda: work.halve(2))
        on(8, lambda: work.halve(3))
        on(9, lambda: work.halve(4))
        on(10, work.turn)

    o = o_ref[...]
    mid = h_ref[...]
    if last:
        mid = mid + dot(o, wo_ref[...]).astype(BF16)
    wide = mid.astype(F32)
    scale = scale_of(wide)
    b = (wide * scale).astype(BF16)
    dy = dy_ref[...]
    b_t, dy_t = b.T, dy.T
    db_s[...] = jnp.zeros_like(db_s)

    def step(c, _):
        talk(c)
        here = pl.ds(pl.multiple_of(c * chunk, chunk), chunk)
        wg, wu = wg_ref[:, here], wu_ref[:, here]
        gate, up = dot(b, wg), dot(b, wu)
        dact = dot(dy, wd_ref[here, :], True).astype(BF16).astype(F32)
        sig = jax.nn.sigmoid(gate)
        silu = gate * sig
        act = (silu * up).astype(BF16)
        dwd_s[:, here] += dot(dy_t, act)
        dgate = (dact * up * (sig + silu - silu * sig)).astype(BF16)
        dup = (dact * silu).astype(BF16)
        dwg_s[:, here] += dot(b_t, dgate)
        dwu_s[:, here] += dot(b_t, dup)
        db_s[...] += dot(dgate, wg, True) + dot(dup, wu, True)

    lax.fori_loop(0, wg_ref.shape[1] // chunk, step, None)
    by = db_s[...].astype(BF16).astype(F32)
    dmid = dy + norm_back(wide, scale, by).astype(BF16)
    dmid_ref[...] = dmid
    dwo_s[...] += dot(o.T, dmid)
    do = dot(dmid, wo_ref[...], True).astype(BF16)
    do_ref[...] = do
    for h in range(delta_ref.shape[0]):
        here = slice(h * HEAD, (h + 1) * HEAD)
        delta_ref[h : h + 1, :] = jnp.sum((do[:, here].astype(F32) * o[:, here].astype(F32)).T, axis=0, keepdims=True)

    @pl.when(step_of == pl.num_programs(0) - 1)
    def _():
        d, many = dwo_s.shape[1], wg_ref.shape[1] // wg_ref.shape[0]
        for c in range(many):
            here = slice(c * d, (c + 1) * d)
            grads_ref[here, :] = dwg_s[:, here].astype(BF16)
            grads_ref[(many + c) * d : (many + c + 1) * d, :] = dwu_s[:, here].astype(BF16)
            grads_ref[(2 * many + c) * d : (2 * many + c + 1) * d, :] = dwd_s[:, here].astype(BF16).T
        grads_ref[3 * many * d :, :] = dwo_s[...].astype(BF16)
        if n:
            wait(work.along(4, True))
            give.start()
            give.wait()


def mlp_back(h, dy, o, wo, wg, wu, wd, number, last, early=(), n=0):
    t, d = h.shape
    sizes = [g.shape[0] for g in early]
    units = sum(sizes)
    of_units = lambda many: ((many, *early[0].shape[1:]), BF16)
    rows = fit(t, ROWS)
    ff, heads = wg.shape[2], o.shape[1] // HEAD
    grads = (3 * ff + o.shape[1], d)
    return pl.pallas_call(
        functools.partial(_mlp_back, chunk=fit(ff, TALK_CHUNK if n else CHUNK), last=last, n=n, sizes=sizes),
        grid=(t // rows,),
        in_specs=[rows_of(d, rows), rows_of(d, rows), rows_of(o.shape[1], rows)] + [of_layer(w, number) for w in (wo, wg, wu, wd)] + [ANY] * len(early),
        out_specs=[rows_of(d, rows), rows_of(o.shape[1], rows), pl.BlockSpec((heads, rows), lambda i: (0, i)), whole(grads)] + [ANY] * bool(n),
        out_shape=[jax.ShapeDtypeStruct((t, d), BF16), jax.ShapeDtypeStruct(o.shape, BF16), jax.ShapeDtypeStruct((heads, t), F32),
                   jax.ShapeDtypeStruct(grads, BF16)] + ([jax.ShapeDtypeStruct(*of_units(units // 16))] if n else []),
        scratch_shapes=[pltpu.VMEM((rows, d), F32), pltpu.VMEM((o.shape[1], d), F32)] + [pltpu.VMEM((d, ff), F32)] * 3
        + ([pltpu.VMEM(*of_units(k)) for k in (units, units // 16, landing(units))] + [pltpu.SemaphoreType.DMA(TALK), pltpu.SemaphoreType.DMA((3,))] if n else []),
        compiler_params=params("arbitrary", talks=1 if n else None),
        name="mlp_back",
    )(h, dy, o, wo, wg, wu, wd, *early)


def _project_back(*refs, first):
    if first:
        h_ref, dq_ref, dk_ref, dv_ref, cos_ref, sin_ref, grads_ref, dwq_s, dwk_s, dwv_s, by_s, bk_s = refs
    else:
        (h_ref, dq_ref, dk_ref, dv_ref, cos_ref, sin_ref, dmid_ref, wq_ref, wk_ref, wv_ref,
         grads_ref, dh_ref, dwq_s, dwk_s, dwv_s, by_s, bk_s) = refs
    step_of = pl.program_id(0)

    @pl.when(step_of == 0)
    def _():
        for s in (dwq_s, dwk_s, dwv_s):
            s[...] = jnp.zeros_like(s)

    wide = h_ref[...].astype(F32)
    scale = scale_of(wide)
    a_t = (wide * scale).astype(BF16).T
    cos, sin = cos_ref[...], sin_ref[...]
    for g_ref, s in ((dq_ref, by_s), (dk_ref, bk_s)):
        for at in range(0, s.shape[1], HEAD):
            here = slice(at, at + HEAD)
            s[:, here] = unturn(g_ref[:, here].astype(F32), cos, sin).astype(BF16)
    dq, dk, dv = by_s[...], bk_s[...], dv_ref[...]
    dwq_s[...] += dot(a_t, dq)
    dwk_s[...] += dot(a_t, dk)
    dwv_s[...] += dot(a_t, dv)
    if not first:
        by = dot(dq, wq_ref[...], True) + dot(dk, wk_ref[...], True) + dot(dv, wv_ref[...], True)
        dh_ref[...] = dmid_ref[...] + norm_back(wide, scale, by.astype(BF16).astype(F32)).astype(BF16)

    @pl.when(step_of == pl.num_programs(0) - 1)
    def _():
        d, nk = dwk_s.shape
        grads_ref[:d, :] = dwq_s[...].astype(BF16)
        grads_ref[d:, :nk] = dwk_s[...].astype(BF16)
        grads_ref[d:, nk:] = dwv_s[...].astype(BF16)


def project_back(h, dq, dk, dv, cos, sin, dmid, wq, wk, wv, number, first):
    t, d = h.shape
    rows = fit(t, ROWS)
    nq, nk = dq.shape[1], dk.shape[1]
    grads = [(d, nq), (d, nk), (d, nk)]
    more = [] if first else [dmid, wq, wk, wv]
    return pl.pallas_call(
        functools.partial(_project_back, first=first),
        grid=(t // rows,),
        in_specs=[rows_of(d, rows), rows_of(nq, rows), rows_of(nk, rows), rows_of(nk, rows), rows_of(HEAD, rows), rows_of(HEAD, rows)]
        + ([] if first else [rows_of(d, rows)] + [of_layer(w, number) for w in (wq, wk, wv)]),
        out_specs=[whole((2 * d, nq))] + ([] if first else [rows_of(d, rows)]),
        out_shape=[jax.ShapeDtypeStruct((2 * d, nq), BF16)] + ([] if first else [jax.ShapeDtypeStruct((t, d), BF16)]),
        scratch_shapes=[pltpu.VMEM(s, F32) for s in grads] + [pltpu.VMEM((rows, nq), BF16), pltpu.VMEM((rows, nk), BF16)],
        compiler_params=params("arbitrary"),
        name="project_back",
    )(h, dq, dk, dv, cos, sin, *more)


def tables(tokens, low=64):
    half = HEAD // 2
    rate = THETA ** (-(jnp.arange(HEAD, dtype=F32) % half) / half)
    sign = jnp.where(jnp.arange(HEAD) < half, -1.0, 1.0)
    high = (low * jnp.arange(tokens // low, dtype=F32))[:, None, None] * rate
    near = jnp.arange(low, dtype=F32)[None, :, None] * rate
    ch, sh, cn, sn = jnp.cos(high), jnp.sin(high), jnp.cos(near), jnp.sin(near)
    return (ch * cn - sh * sn).reshape(tokens, HEAD), (sign * (sh * cn + ch * sn)).reshape(tokens, HEAD)


def _last_sum(*refs, n, sizes):
    (early_ref, late_ref, done_ref), (out_ref, squares_ref), (grads, sums, done, lands, sems, local) = refs[:3], refs[3:5], refs[5:]
    units = sizes[0] + sizes[1]
    work = GroupSum(grads, sums, units, lands, sems, n)
    loads = local_copies([(early_ref, grads.at[pl.ds(0, sizes[0])]), (late_ref, grads.at[pl.ds(*sizes[:2])]), (done_ref, done)], local)
    gives = local_copies([(done, out_ref.at[pl.ds(units, sizes[2])])]
                         + [(sums.at[pl.ds(first, work.half)], out_ref.at[pl.ds(first, work.half)]) for first in (work.mine, work.other)], local, 3)
    start(loads)
    greet(work.partner)
    wait(loads[:2])
    many = 4

    def squares(ref, first, size):
        def step(i, total):
            g = ref[pl.ds(first + i * many, many)].astype(F32)
            return total + jnp.sum(g * g, axis=0)

        return lax.fori_loop(0, size // many, step, jnp.zeros(ref.shape[1:], F32))

    work.halve(0)
    wait(loads[2:])
    start(gives[:1])
    work.halve(1)
    total = squares(done, 0, sizes[2])
    work.halve(2)
    work.halve(3)
    work.halve(4)
    work.turn()
    work.double(3)
    work.double(2)
    work.double(1)
    work.double(0)
    start(gives[1:2])
    mine = squares(sums, work.mine, work.half)
    work.end()
    start(gives[2:])
    total = total + (mine + squares(sums, work.other, work.half))
    squares_ref[...] = jnp.full(squares_ref.shape, jnp.sum(total))
    wait(gives)


def last_sum(grads, n):
    sizes = [g.shape[0] for g in grads]
    total, mine, unit = sum(sizes), sizes[0] + sizes[1], grads[0].shape[1:]
    out, squares = pl.pallas_call(
        functools.partial(_last_sum, n=n, sizes=sizes),
        in_specs=[ANY] * len(grads),
        out_specs=[ANY, pl.BlockSpec(memory_space=pltpu.VMEM)],
        out_shape=[jax.ShapeDtypeStruct((total, *unit), BF16), jax.ShapeDtypeStruct((8, 128), F32)],
        scratch_shapes=[pltpu.VMEM((k, *unit), BF16) for k in (mine, mine, total - mine, landing(mine))]
        + [pltpu.SemaphoreType.DMA(TALK), pltpu.SemaphoreType.DMA((6,))],
        compiler_params=params(talks=0),
        name="last_sum",
    )(*grads)
    return out.reshape(-1, unit[-1]), squares


def _adamw(squares_ref, *refs, many, count):
    factor = jnp.minimum(1.0, 0.5 * lax.rsqrt(squares_ref[0:1, 0:1] / count + 1e-30))
    for i in range(many):
        w, m, v, g = (refs[4 * i + j][...].astype(F32) for j in range(4))
        g = g * factor
        m = 0.9 * m + 0.1 * g
        v = 0.95 * v + 0.05 * g * g
        w_out, m_out, v_out = refs[4 * many + 3 * i : 4 * many + 3 * i + 3]
        w_out[...] = (w - 0.02 * (m * lax.rsqrt(v + 1e-8) + 0.1 * w)).astype(BF16)
        m_out[...] = m
        v_out[...] = v


def adamw(squares, grads, items, grid, count, name):
    ins, specs, outs, shapes = [squares], [whole(squares.shape)], [], []
    for w, m, v, spec, g_spec in items:
        ins += [w, m, v, grads]
        specs += [spec, spec, spec, g_spec]
        outs += [spec] * 3
        shapes += [jax.ShapeDtypeStruct(x.shape, x.dtype) for x in (w, m, v)]
    size = sum(x[0].size for x in items)
    new = pl.pallas_call(
        functools.partial(_adamw, many=len(items), count=count),
        grid=grid,
        in_specs=specs,
        out_specs=outs,
        out_shape=shapes,
        compiler_params=params(*["arbitrary"] * len(grid)),
        name=name,
    )(*ins)
    return [new[3 * i : 3 * i + 3] for i in range(len(items))]


def optimizer(weights, m, v, grads, squares):
    layers, d, ff = weights[4].shape
    n = ff // d
    pieces = 3 * n + 3
    count = sum(w.size for w in weights)
    rows = fit(d, STEP)
    of_d = d // rows
    wide = pl.BlockSpec((None, rows, d), lambda l, c, r: (l, r, c))
    tall = pl.BlockSpec((None, rows, d), lambda l, c, r: (l, c * of_d + r, 0))
    piece = lambda first: pl.BlockSpec((rows, d), lambda l, c, r: ((l * pieces + first + c) * of_d + r, 0))
    big = adamw(squares, grads, [(weights[i], m[i], v[i], spec, piece(at)) for i, spec, at in ((4, wide, 0), (5, wide, n), (6, tall, n + n))],
                (layers, n, of_d), count, "adamw_mlp")
    nk = weights[1].shape[2]
    row = lambda width: pl.BlockSpec((None, rows // 2, width), lambda l, r: (l, r, 0))
    part = lambda at, width, col: pl.BlockSpec((rows // 2, width), lambda l, r: ((l * pieces + at) * of_d * 2 + r, col))
    small = adamw(squares, grads, [(weights[i], m[i], v[i], row(width), part(pieces - at, width, col)) for i, width, at, col in
                                   ((0, d, 2, 0), (1, nk, 1, 0), (2, nk, 1, 1), (3, d, 3, 0))],
                  (layers, of_d * 2), count, "adamw_attention")
    return small + big


def solution(mesh):
    def step(x, dy, *arrays):
        weights, m, v = (arrays[i * len(NAMES) : (i + 1) * len(NAMES)] for i in range(3))
        wq, wk, wv, wo, wg, wu, wd = weights
        layers = wq.shape[0]
        cos, sin = tables(x.shape[1])
        h, kept = x[0], []
        for n in range(layers):
            q, k, val = project(h, wq, wk, wv, cos, sin, n)
            o, lse = attend(q, k, val)
            last = n == layers - 1
            mid, out = (h, None) if last else mlp(h, o, wo, wg, wu, wd, n)
            kept.append((h, q, k, val, o, lse, mid))
            h = out
        by_h, early, sums, size = dy[0], (), [], mesh.shape["dp"]
        for n in reversed(range(layers)):
            h, q, k, val, o, lse, mid = kept[n]
            group = size if early else 0
            dmid, do, delta, mine, *part = mlp_back(mid, by_h, o, wo, wg, wu, wd, n, n == layers - 1, early, group)
            dq, dk, dv, *done = attend_back(q, k, val, do, lse, delta, *part, units=sum(g.shape[0] for g in early), n=group)
            qkv, *rest = project_back(h, dq, dk, dv, cos, sin, dmid, wq, wk, wv, n, n == 0)
            by_h = rest[0] if rest else None
            sums = done + sums
            early = tuple(g.reshape(-1, UNIT, g.shape[1]) for g in (mine, qkv))
        grads, squares = last_sum([*early, jnp.concatenate(sums) if len(sums) > 1 else sums[0]], size)
        new = optimizer(weights, m, v, grads, squares)
        return tuple(one[which] for which in range(3) for one in new)

    states, all_of = P(("rep", "dp")), P()
    return jax.shard_map(
        step,
        mesh=mesh,
        in_specs=(states, states) + (all_of,) * 21,
        out_specs=(P("rep"),) * 21,
        check_vma=False,
    )
```

```python
import functools
import math

import jax
import jax.numpy as jnp
from jax import lax
from jax.experimental import pallas as pl
from jax.experimental.pallas import tpu as pltpu
from jax.sharding import PartitionSpec as P

HEAD = 128
THETA = 10000
NAMES = ("wq", "wk", "wv", "wo", "w_gate", "w_up", "w_down")
NEG = -1e30
HIDDEN = 2 * NEG
LOG2E = 1.4426950408889634
VMEM = 66060288
F32, BF16 = jnp.float32, jnp.bfloat16

ROWS = 512
CHUNK, TALK_CHUNK = 1536, 512
QUERIES = 1024
KEYS, BACK_KEYS = 512, 256
STEP = 512


def fit(size, want, unit=128):
    return max(n for n in range(unit, max(min(want, size), unit) + 1, unit) if size % n == 0)


def dot(a, b, turned=False):
    return lax.dot_general(a, b, (((1,), (int(turned),)), ((), ())), preferred_element_type=F32)


def scale_of(wide):
    return lax.rsqrt(jnp.mean(wide * wide, -1, keepdims=True) + 1e-6)


def norm_back(wide, scale, by):
    return scale * (by - wide * (scale * scale * jnp.mean(by * wide, -1, keepdims=True)))


def turn(t, cos, sin):
    return t * cos + pltpu.roll(t, HEAD // 2, 1) * sin


def unturn(t, cos, sin):
    return t * cos - pltpu.roll(t, HEAD // 2, 1) * sin


def params(*semantics, talks=None):
    more = {} if talks is None else {"collective_id": talks, "has_side_effects": True}
    return pltpu.CompilerParams(dimension_semantics=semantics, vmem_limit_bytes=VMEM, **more)


ANY = pl.BlockSpec(memory_space=pl.ANY)


def at(slot, when, *actions):
    @pl.when(slot == when)
    def _():
        for action in actions:
            action()


def whole(shape):
    return pl.BlockSpec(shape, lambda *_: (0,) * len(shape))


def of_layer(w, number):
    return pl.BlockSpec((None, *w.shape[1:]), lambda *_: (number, 0, 0), pipeline_mode=pl.Buffered(1))


def rows_of(width, rows):
    return pl.BlockSpec((rows, width), lambda i: (i, 0))


TALK = (2, 2, 6, 4)
UNIT = 16


def places(n):
    side = math.isqrt(n // 2)
    me = lax.axis_index("dp")
    core, y, x = lax.rem(me, 2), lax.rem(lax.div(me, 2), side), lax.div(me, 2 * side)
    at = lambda x, y: (x * side + y) * 2 + core
    near = lambda a: a + 1 - 2 * lax.rem(a, 2)
    bit = lambda a: lax.rem(lax.div(a + 1, 2), 2)
    return [(me + 1 - 2 * core, core), (at(near(x), y), bit(x)), (at(x, near(y)), bit(y)),
            (at(side - 1 - x, y), lax.div(x, 2)), (at(x, side - 1 - y), lax.div(y, 2))]


class GroupSum:
    def __init__(self, grads, out, units, lands, sems, n, compact=False):
        self.grads, self.out, self.lands, self.sems = grads, out, lands, sems
        spots = places(n)
        self.partner = [device for device, _ in spots]
        half = units // 2
        self.half, self.mine, self.other = half, spots[0][1] * half, (1 - spots[0][1]) * half
        land, offs, size = half, [self.mine + q * (half // 4) for q in range(4)], half // 4
        self.steps = [None]
        for k in range(4):
            size //= 2
            now = []
            for q in range(4):
                dim = 1 + (q + k) % 4
                bit = spots[dim][1]
                now.append((self.partner[dim], offs[q] + (1 - bit) * size, offs[q] + bit * size, size, land))
                offs[q] = offs[q] + bit * size
                land += size
            self.steps.append(now)
        first = [kept for _, _, kept, _, _ in self.steps[3]]
        self.moved = (lambda q, where: q * 2 * size + where - first[q]) if compact else (lambda q, where: where)

    def remote(self, src, dst, row, q, device, out):
        return pltpu.make_async_remote_copy(src, dst, self.sems.at[int(out), 0, row, q], self.sems.at[int(out), 1, row, q],
                                            device_id={"dp": device}, device_id_type=pl.DeviceIdType.MESH)

    def across(self, part, out):
        made = []
        for q, step in enumerate(self.steps[1]):
            where, size = step[1 + part], step[3]
            if out:
                src = dst = self.out.at[pl.ds(where, size)]
            else:
                src, dst = self.grads.at[pl.ds(where - self.mine + self.other, size)], self.lands.at[pl.ds(where - self.mine, size)]
            made.append(self.remote(src, dst, 5 * part, q, self.partner[0], out))
        return made

    def along(self, k, out):
        made = []
        for q, (device, sent, kept, size, land) in enumerate(self.steps[k]):
            if out:
                src = dst = self.out.at[pl.ds(self.moved(q, kept), size)]
            else:
                src, dst = self.grads.at[pl.ds(sent, size)], self.lands.at[pl.ds(land, size)]
            made.append(self.remote(src, dst, k, q, device, out))
        return made

    def add(self, to, where, land, size, into=None):
        many = math.gcd(size, 12)
        into = where if into is None else into

        def step(i, _):
            total = self.grads[pl.ds(where + i * many, many)].astype(F32) + self.lands[pl.ds(land + i * many, many)].astype(F32)
            to[pl.ds(into + i * many, many)] = total.astype(BF16)

        lax.fori_loop(0, size // many, step, None)

    def halve(self, k):
        if k == 0:
            start(self.across(0, False) + self.across(1, False))
        elif k == 1:
            wait(self.across(0, False))
            for _, sent, kept, size, _ in self.steps[1]:
                self.add(self.grads, sent, sent - self.mine, size)
            start(self.along(1, False))
            wait(self.across(1, False))
            for _, sent, kept, size, _ in self.steps[1]:
                self.add(self.grads, kept, kept - self.mine, size)
        else:
            wait(self.along(k - 1, False))
            for part in (1, 2):
                for now, (_, _, before, _, land) in zip(self.steps[k], self.steps[k - 1]):
                    self.add(self.grads, now[part], land + now[part] - before, now[3])
                if part == 1:
                    start(self.along(k, False))

    def turn(self):
        wait(self.along(4, False))
        for q, (_, _, kept, size, land) in enumerate(self.steps[4]):
            self.add(self.out, kept, land, size, self.moved(q, kept))
        start(self.along(4, True))

    def double(self, k, begin=False):
        if not begin:
            wait(self.along(k + 1, True))
        start(self.along(k, True) if k else self.across(0, True))
        if k == 1:
            start(self.across(1, True))

    def end(self):
        wait(self.across(0, True) + self.across(1, True))

    def after(self, k):
        return [(kept, size) for _, _, kept, size, _ in self.steps[k]]


def start(copies):
    for copy in copies:
        copy.start()


def wait(copies):
    for copy in copies:
        copy.wait()


def landing(units):
    return units - units // 32


def local_copies(pairs, sems, first=0):
    return [pltpu.make_async_copy(src, dst, sems.at[first + i]) for i, (src, dst) in enumerate(pairs)]


def greet(partners):
    barrier = pltpu.get_barrier_semaphore()
    for device in partners:
        pl.semaphore_signal(barrier, inc=1, device_id={"dp": device}, device_id_type=pl.DeviceIdType.MESH)
    pl.semaphore_wait(barrier, len(partners))


def _project(h_ref, wq_ref, wk_ref, wv_ref, cos_ref, sin_ref, q_ref, k_ref, v_ref):
    wide = h_ref[...].astype(F32)
    a = (wide * scale_of(wide)).astype(BF16)
    cos, sin = cos_ref[...], sin_ref[...]
    for w_ref, o_ref in ((wq_ref, q_ref), (wk_ref, k_ref)):
        t = dot(a, w_ref[...]).astype(BF16).astype(F32)
        for at in range(0, t.shape[1], HEAD):
            o_ref[:, at : at + HEAD] = turn(t[:, at : at + HEAD], cos, sin).astype(BF16)
    v_ref[...] = dot(a, wv_ref[...]).astype(BF16)


def project(h, wq, wk, wv, cos, sin, number):
    t, d = h.shape
    rows = fit(t, 2 * ROWS)
    dq, dk = wq.shape[2], wk.shape[2]
    return pl.pallas_call(
        _project,
        grid=(t // rows,),
        in_specs=[rows_of(d, rows), of_layer(wq, number), of_layer(wk, number), of_layer(wv, number), rows_of(HEAD, rows), rows_of(HEAD, rows)],
        out_specs=[rows_of(dq, rows), rows_of(dk, rows), rows_of(dk, rows)],
        out_shape=[jax.ShapeDtypeStruct((t, n), BF16) for n in (dq, dk, dk)],
        compiler_params=params("arbitrary"),
        name="project",
    )(h, wq, wk, wv, cos, sin)


def _diagonal(bq, bk, wide):
    out = []
    for m in range(-(-bq // bk)):
        out.append((m, {r: m * bk + bk - 1 > r for r in range(0, bq, wide) if m * bk < r + wide}))
    return out


def _attend(q_ref, k_ref, v_ref, o_ref, lse_ref, top_s, mix_s, *, scale, bq, bk, wide, kv, g):
    iq = pl.program_id(0)
    e = scale * LOG2E
    pieces = [(p, i, i * g + n, r) for p, (i, n, r) in
              enumerate((i, n, r) for i in range(kv) for n in range(g) for r in range(0, bq, wide))]
    top_s[...] = jnp.full(top_s.shape, NEG, F32)
    mix_s[...] = jnp.zeros(mix_s.shape, F32)
    ones = jnp.ones((8, bk), BF16)
    gap = lax.broadcasted_iota(jnp.int32, (bk, wide), 1) - lax.broadcasted_iota(jnp.int32, (bk, wide), 0)

    def block(j, strips, m=0):
        here = pl.ds(pl.multiple_of(j * bk, bk), bk)
        now = [x for x in pieces if strips is None or x[3] in strips]
        scores = [dot(k_ref[here, i * HEAD : (i + 1) * HEAD], q_ref[r : r + wide, h * HEAD : (h + 1) * HEAD], True) for _, i, h, r in now]
        weights, keeps = [], []
        for (p, i, h, r), s in zip(now, scores):
            if strips is not None and strips[r]:
                s = jnp.where(gap >= m * bk - r, s, HIDDEN)
            old = top_s[p : p + 1, :]
            top = jnp.maximum(old, s.max(axis=0, keepdims=True))
            top_s[p : p + 1, :] = top
            weights.append(jnp.exp2((s - top) * e).astype(BF16))
            keeps.append(jnp.exp2((old - top) * e))
        values = [jnp.concatenate([v_ref[here, i * HEAD : (i + 1) * HEAD].T, ones], axis=0) for i in range(kv)]
        for (p, i, h, r), w, keep in zip(now, weights, keeps):
            mix_s[p] = mix_s[p] * keep + dot(values[i], w)

    first = lax.div(iq * bq, bk)
    lax.fori_loop(0, first, lambda j, _: block(j, None), None)
    for m, strips in _diagonal(bq, bk, wide):
        block(first + m, strips, m)
    for p, i, h, r in pieces:
        total = mix_s[p, HEAD : HEAD + 1, :]
        o_ref[r : r + wide, h * HEAD : (h + 1) * HEAD] = (mix_s[p, :HEAD, :] * (1 / total)).T.astype(BF16)
        lse_ref[h : h + 1, r : r + wide] = top_s[p : p + 1, :] * scale + jnp.log(total)


def attend(q, k, v):
    t = q.shape[0]
    heads, kv = q.shape[1] // HEAD, k.shape[1] // HEAD
    bq = fit(t, QUERIES)
    bk = wide = fit(bq, KEYS)
    n = heads * (bq // wide)
    return pl.pallas_call(
        functools.partial(_attend, scale=HEAD**-0.5, bq=bq, bk=bk, wide=wide, kv=kv, g=heads // kv),
        grid=(t // bq,),
        in_specs=[rows_of(q.shape[1], bq), whole(k.shape), whole(v.shape)],
        out_specs=[rows_of(q.shape[1], bq), pl.BlockSpec((heads, bq), lambda i: (0, i))],
        out_shape=[jax.ShapeDtypeStruct(q.shape, BF16), jax.ShapeDtypeStruct((heads, t), F32)],
        scratch_shapes=[pltpu.VMEM((n, wide), F32), pltpu.VMEM((n, HEAD + 8, wide), F32)],
        compiler_params=params("arbitrary"),
        name="attend",
    )(q, k, v)


def _attend_back(q_ref, k_ref, v_ref, do_ref, lse_ref, delta_ref, *refs, scale, bq, bk, wide, kv, g, n):
    iq = pl.program_id(0)
    if n:
        part_ref, dq_ref, dk_ref, dv_ref, sum_ref, dq_s, dk_s, dv_s, sum_s, sems, local = refs
        work = GroupSum(None, sum_s, sum_s.shape[0], None, sems, n)
        takes = local_copies([(part_ref.at[pl.ds(q * size, size)], sum_s.at[pl.ds(first, size)]) for q, (first, size) in enumerate(work.after(3))], local)
        gives = local_copies([(sum_s.at[pl.ds(first, work.half)], sum_ref.at[pl.ds(first, work.half)]) for first in (work.mine, work.other)], local, 4)
    else:
        dq_ref, dk_ref, dv_ref, dq_s, dk_s, dv_s = refs

    e = scale * LOG2E
    pieces = [(i, i * g + n, r) for i in range(kv) for n in range(g) for r in range(0, bq, wide)]

    @pl.when(iq == 0)
    def _():
        dk_s[...] = jnp.zeros_like(dk_s)
        dv_s[...] = jnp.zeros_like(dv_s)

    dq_s[...] = jnp.zeros_like(dq_s)
    gap = lax.broadcasted_iota(jnp.int32, (bk, wide), 1) - lax.broadcasted_iota(jnp.int32, (bk, wide), 0)

    def block(j, strips, m=0):
        here = pl.ds(pl.multiple_of(j * bk, bk), bk)
        now = [x for x in pieces if strips is None or x[2] in strips]
        col = lambda n: slice(n * HEAD, (n + 1) * HEAD)
        qs = [q_ref[r : r + wide, col(h)] for _, h, r in now]
        dos = [do_ref[r : r + wide, col(h)] for _, h, r in now]
        scores = [dot(k_ref[here, col(i)], x, True) for (i, _, _), x in zip(now, qs)]
        dps = [dot(v_ref[here, col(i)], x, True) for (i, _, _), x in zip(now, dos)]
        turned = [k_ref[here, col(i)].T for i in range(kv)]
        for (i, h, r), q, do, s, dp in zip(now, qs, dos, scores, dps):
            p = jnp.exp2(s * e - lse_ref[h : h + 1, r : r + wide] * LOG2E)
            if strips is not None and strips[r]:
                p = jnp.where(gap >= m * bk - r, p, 0.0)
            ds = (p * (dp - delta_ref[h : h + 1, r : r + wide])).astype(BF16)
            dv_s[i, here, :] += dot(p.astype(BF16), do)
            dk_s[i, here, :] += dot(ds, q)
            dq_s[h, :, r : r + wide] += dot(turned[i], ds)

    first = lax.div(iq * bq, bk)
    last = pl.num_programs(0) - 1

    def loop(j, _):
        if n:
            at(iq * bq + j, last * bq + 1, lambda: work.double(1))
        block(j, None)

    if n:
        at(iq, 0, lambda: start(takes), lambda: greet(work.partner), lambda: wait(takes), lambda: work.double(3, True))
    lax.fori_loop(0, first, loop, None)
    for m, strips in _diagonal(bq, bk, wide):
        if n and m == 1:
            at(iq, last, lambda: work.double(0), lambda: gives[0].start())
        if n and m == 2:
            at(iq, 0, lambda: work.double(2))
        block(first + m, strips, m)
    for h in range(kv * g):
        dq_ref[:, h * HEAD : (h + 1) * HEAD] = (dq_s[h] * scale).T.astype(BF16)

    @pl.when(iq == last)
    def _():
        for i in range(kv):
            dk_ref[:, i * HEAD : (i + 1) * HEAD] = (dk_s[i] * scale).astype(BF16)
            dv_ref[:, i * HEAD : (i + 1) * HEAD] = dv_s[i].astype(BF16)
        if n:
            work.end()
            gives[1].start()
            wait(gives)


def attend_back(q, k, v, do, lse, delta, part=None, units=0, n=0):
    t = q.shape[0]
    heads, kv = q.shape[1] // HEAD, k.shape[1] // HEAD
    bq = fit(t, QUERIES)
    bk = wide = fit(bq, BACK_KEYS)
    stats = pl.BlockSpec((heads, bq), lambda i: (0, i))
    return pl.pallas_call(
        functools.partial(_attend_back, scale=HEAD**-0.5, bq=bq, bk=bk, wide=wide, kv=kv, g=heads // kv, n=n),
        grid=(t // bq,),
        in_specs=[rows_of(q.shape[1], bq), whole(k.shape), whole(v.shape), rows_of(q.shape[1], bq), stats, stats] + [ANY] * bool(n),
        out_specs=[rows_of(q.shape[1], bq), whole(k.shape), whole(v.shape)] + [ANY] * bool(n),
        out_shape=[jax.ShapeDtypeStruct(x.shape, BF16) for x in (q, k, v)] + ([jax.ShapeDtypeStruct((units, *part.shape[1:]), BF16)] if n else []),
        scratch_shapes=[pltpu.VMEM((heads, HEAD, bq), F32), pltpu.VMEM((kv, t, HEAD), F32), pltpu.VMEM((kv, t, HEAD), F32)]
        + ([pltpu.VMEM((units, *part.shape[1:]), BF16), pltpu.SemaphoreType.DMA(TALK), pltpu.SemaphoreType.DMA((6,))] if n else []),
        compiler_params=params("arbitrary", talks=2 if n else None),
        name="attend_back",
    )(q, k, v, do, lse, delta, *([part] if n else []))


def _mlp(h_ref, o_ref, wo_ref, wg_ref, wu_ref, wd_ref, mid_ref, out_ref, acc_s, *, chunk):
    mid = h_ref[...] + dot(o_ref[...], wo_ref[...]).astype(BF16)
    mid_ref[...] = mid
    wide = mid.astype(F32)
    b = (wide * scale_of(wide)).astype(BF16)
    acc_s[...] = jnp.zeros_like(acc_s)

    def step(c, _):
        here = pl.ds(pl.multiple_of(c * chunk, chunk), chunk)
        gate, up = dot(b, wg_ref[:, here]), dot(b, wu_ref[:, here])
        acc_s[...] += dot((gate * jax.nn.sigmoid(gate) * up).astype(BF16), wd_ref[here, :])

    lax.fori_loop(0, wg_ref.shape[1] // chunk, step, None)
    out_ref[...] = mid + acc_s[...].astype(BF16)


def mlp(h, o, wo, wg, wu, wd, number):
    t, d = h.shape
    rows = fit(t, ROWS)
    ff = wg.shape[2]
    return pl.pallas_call(
        functools.partial(_mlp, chunk=fit(ff, CHUNK)),
        grid=(t // rows,),
        in_specs=[rows_of(d, rows), rows_of(o.shape[1], rows)] + [of_layer(w, number) for w in (wo, wg, wu, wd)],
        out_specs=[rows_of(d, rows)] * 2,
        out_shape=[jax.ShapeDtypeStruct((t, d), BF16)] * 2,
        scratch_shapes=[pltpu.VMEM((rows, d), F32)],
        compiler_params=params("arbitrary"),
        name="mlp",
    )(h, o, wo, wg, wu, wd)


def _mlp_back(*refs, chunk, last, n, sizes):
    if n:
        (*ins, early_ref, late_ref), outs, scratch = refs[:9], refs[9:14], refs[14:]
        (*outs, part_ref), (*scratch, sum_s, part_s, lands, sems, local) = outs, scratch
        refs = (*ins, *outs, *scratch)
    (h_ref, dy_ref, o_ref, wo_ref, wg_ref, wu_ref, wd_ref,
     dmid_ref, do_ref, delta_ref, grads_ref, db_s, dwo_s, dwg_s, dwu_s, dwd_s) = refs
    step_of = pl.program_id(0)

    @pl.when(step_of == 0)
    def _():
        for s in (dwo_s, dwg_s, dwu_s, dwd_s):
            s[...] = jnp.zeros_like(s)

    if n:
        work = GroupSum(sum_s, part_s, sum(sizes), lands, sems, n, compact=True)
        loads = local_copies([(early_ref, sum_s.at[pl.ds(0, sizes[0])]), (late_ref, sum_s.at[pl.ds(*sizes)])], local)
        give = pltpu.make_async_copy(part_s, part_ref, local.at[2])

    def talk(c):
        if not n:
            return
        chunks = wg_ref.shape[1] // chunk
        slot, slots = step_of * chunks + c, pl.num_programs(0) * chunks
        on = lambda when, *actions: at(slot, lax.div(when * slots, 12), *actions)
        on(0, lambda: start(loads), lambda: greet(work.partner))
        on(1, lambda: wait(loads), lambda: work.halve(0))
        on(3, lambda: work.halve(1))
        on(6, lambda: work.halve(2))
        on(8, lambda: work.halve(3))
        on(9, lambda: work.halve(4))
        on(10, work.turn)

    o = o_ref[...]
    mid = h_ref[...]
    if last:
        mid = mid + dot(o, wo_ref[...]).astype(BF16)
    wide = mid.astype(F32)
    scale = scale_of(wide)
    b = (wide * scale).astype(BF16)
    dy = dy_ref[...]
    b_t, dy_t = b.T, dy.T
    db_s[...] = jnp.zeros_like(db_s)

    def step(c, _):
        talk(c)
        here = pl.ds(pl.multiple_of(c * chunk, chunk), chunk)
        wg, wu = wg_ref[:, here], wu_ref[:, here]
        gate, up = dot(b, wg), dot(b, wu)
        dact = dot(dy, wd_ref[here, :], True).astype(BF16).astype(F32)
        sig = jax.nn.sigmoid(gate)
        silu = gate * sig
        act = (silu * up).astype(BF16)
        dwd_s[:, here] += dot(dy_t, act)
        dgate = (dact * up * (sig + silu - silu * sig)).astype(BF16)
        dup = (dact * silu).astype(BF16)
        dwg_s[:, here] += dot(b_t, dgate)
        dwu_s[:, here] += dot(b_t, dup)
        db_s[...] += dot(dgate, wg, True) + dot(dup, wu, True)

    lax.fori_loop(0, wg_ref.shape[1] // chunk, step, None)
    by = db_s[...].astype(BF16).astype(F32)
    dmid = dy + norm_back(wide, scale, by).astype(BF16)
    dmid_ref[...] = dmid
    dwo_s[...] += dot(o.T, dmid)
    do = dot(dmid, wo_ref[...], True).astype(BF16)
    do_ref[...] = do
    for h in range(delta_ref.shape[0]):
        here = slice(h * HEAD, (h + 1) * HEAD)
        delta_ref[h : h + 1, :] = jnp.sum((do[:, here].astype(F32) * o[:, here].astype(F32)).T, axis=0, keepdims=True)

    @pl.when(step_of == pl.num_programs(0) - 1)
    def _():
        d, many = dwo_s.shape[1], wg_ref.shape[1] // wg_ref.shape[0]
        for c in range(many):
            here = slice(c * d, (c + 1) * d)
            grads_ref[here, :] = dwg_s[:, here].astype(BF16)
            grads_ref[(many + c) * d : (many + c + 1) * d, :] = dwu_s[:, here].astype(BF16)
            grads_ref[(2 * many + c) * d : (2 * many + c + 1) * d, :] = dwd_s[:, here].astype(BF16).T
        grads_ref[3 * many * d :, :] = dwo_s[...].astype(BF16)
        if n:
            wait(work.along(4, True))
            give.start()
            give.wait()


def mlp_back(h, dy, o, wo, wg, wu, wd, number, last, early=(), n=0):
    t, d = h.shape
    sizes = [g.shape[0] for g in early]
    units = sum(sizes)
    of_units = lambda many: ((many, *early[0].shape[1:]), BF16)
    rows = fit(t, ROWS)
    ff, heads = wg.shape[2], o.shape[1] // HEAD
    grads = (3 * ff + o.shape[1], d)
    return pl.pallas_call(
        functools.partial(_mlp_back, chunk=fit(ff, TALK_CHUNK if n else CHUNK), last=last, n=n, sizes=sizes),
        grid=(t // rows,),
        in_specs=[rows_of(d, rows), rows_of(d, rows), rows_of(o.shape[1], rows)] + [of_layer(w, number) for w in (wo, wg, wu, wd)] + [ANY] * len(early),
        out_specs=[rows_of(d, rows), rows_of(o.shape[1], rows), pl.BlockSpec((heads, rows), lambda i: (0, i)), whole(grads)] + [ANY] * bool(n),
        out_shape=[jax.ShapeDtypeStruct((t, d), BF16), jax.ShapeDtypeStruct(o.shape, BF16), jax.ShapeDtypeStruct((heads, t), F32),
                   jax.ShapeDtypeStruct(grads, BF16)] + ([jax.ShapeDtypeStruct(*of_units(units // 16))] if n else []),
        scratch_shapes=[pltpu.VMEM((rows, d), F32), pltpu.VMEM((o.shape[1], d), F32)] + [pltpu.VMEM((d, ff), F32)] * 3
        + ([pltpu.VMEM(*of_units(k)) for k in (units, units // 16, landing(units))] + [pltpu.SemaphoreType.DMA(TALK), pltpu.SemaphoreType.DMA((3,))] if n else []),
        compiler_params=params("arbitrary", talks=1 if n else None),
        name="mlp_back",
    )(h, dy, o, wo, wg, wu, wd, *early)


def _project_back(*refs, first):
    if first:
        h_ref, dq_ref, dk_ref, dv_ref, cos_ref, sin_ref, grads_ref, dwq_s, dwk_s, dwv_s, by_s, bk_s = refs
    else:
        (h_ref, dq_ref, dk_ref, dv_ref, cos_ref, sin_ref, dmid_ref, wq_ref, wk_ref, wv_ref,
         grads_ref, dh_ref, dwq_s, dwk_s, dwv_s, by_s, bk_s) = refs
    step_of = pl.program_id(0)

    @pl.when(step_of == 0)
    def _():
        for s in (dwq_s, dwk_s, dwv_s):
            s[...] = jnp.zeros_like(s)

    wide = h_ref[...].astype(F32)
    scale = scale_of(wide)
    a_t = (wide * scale).astype(BF16).T
    cos, sin = cos_ref[...], sin_ref[...]
    for g_ref, s in ((dq_ref, by_s), (dk_ref, bk_s)):
        for at in range(0, s.shape[1], HEAD):
            here = slice(at, at + HEAD)
            s[:, here] = unturn(g_ref[:, here].astype(F32), cos, sin).astype(BF16)
    dq, dk, dv = by_s[...], bk_s[...], dv_ref[...]
    dwq_s[...] += dot(a_t, dq)
    dwk_s[...] += dot(a_t, dk)
    dwv_s[...] += dot(a_t, dv)
    if not first:
        by = dot(dq, wq_ref[...], True) + dot(dk, wk_ref[...], True) + dot(dv, wv_ref[...], True)
        dh_ref[...] = dmid_ref[...] + norm_back(wide, scale, by.astype(BF16).astype(F32)).astype(BF16)

    @pl.when(step_of == pl.num_programs(0) - 1)
    def _():
        d, nk = dwk_s.shape
        grads_ref[:d, :] = dwq_s[...].astype(BF16)
        grads_ref[d:, :nk] = dwk_s[...].astype(BF16)
        grads_ref[d:, nk:] = dwv_s[...].astype(BF16)


def project_back(h, dq, dk, dv, cos, sin, dmid, wq, wk, wv, number, first):
    t, d = h.shape
    rows = fit(t, ROWS)
    nq, nk = dq.shape[1], dk.shape[1]
    grads = [(d, nq), (d, nk), (d, nk)]
    more = [] if first else [dmid, wq, wk, wv]
    return pl.pallas_call(
        functools.partial(_project_back, first=first),
        grid=(t // rows,),
        in_specs=[rows_of(d, rows), rows_of(nq, rows), rows_of(nk, rows), rows_of(nk, rows), rows_of(HEAD, rows), rows_of(HEAD, rows)]
        + ([] if first else [rows_of(d, rows)] + [of_layer(w, number) for w in (wq, wk, wv)]),
        out_specs=[whole((2 * d, nq))] + ([] if first else [rows_of(d, rows)]),
        out_shape=[jax.ShapeDtypeStruct((2 * d, nq), BF16)] + ([] if first else [jax.ShapeDtypeStruct((t, d), BF16)]),
        scratch_shapes=[pltpu.VMEM(s, F32) for s in grads] + [pltpu.VMEM((rows, nq), BF16), pltpu.VMEM((rows, nk), BF16)],
        compiler_params=params("arbitrary"),
        name="project_back",
    )(h, dq, dk, dv, cos, sin, *more)


def tables(tokens, low=64):
    half = HEAD // 2
    rate = THETA ** (-(jnp.arange(HEAD, dtype=F32) % half) / half)
    sign = jnp.where(jnp.arange(HEAD) < half, -1.0, 1.0)
    high = (low * jnp.arange(tokens // low, dtype=F32))[:, None, None] * rate
    near = jnp.arange(low, dtype=F32)[None, :, None] * rate
    ch, sh, cn, sn = jnp.cos(high), jnp.sin(high), jnp.cos(near), jnp.sin(near)
    return (ch * cn - sh * sn).reshape(tokens, HEAD), (sign * (sh * cn + ch * sn)).reshape(tokens, HEAD)


def _last_sum(*refs, n, sizes):
    (early_ref, late_ref, done_ref), (out_ref, squares_ref), (grads, sums, done, lands, sems, local) = refs[:3], refs[3:5], refs[5:]
    units = sizes[0] + sizes[1]
    work = GroupSum(grads, sums, units, lands, sems, n)
    loads = local_copies([(early_ref, grads.at[pl.ds(0, sizes[0])]), (late_ref, grads.at[pl.ds(*sizes[:2])]), (done_ref, done)], local)
    gives = local_copies([(done, out_ref.at[pl.ds(units, sizes[2])])]
                         + [(sums.at[pl.ds(first, work.half)], out_ref.at[pl.ds(first, work.half)]) for first in (work.mine, work.other)], local, 3)
    start(loads)
    greet(work.partner)
    wait(loads[:2])
    many = 4

    def squares(ref, first, size):
        def step(i, total):
            g = ref[pl.ds(first + i * many, many)].astype(F32)
            return total + jnp.sum(g * g, axis=0)

        return lax.fori_loop(0, size // many, step, jnp.zeros(ref.shape[1:], F32))

    work.halve(0)
    wait(loads[2:])
    start(gives[:1])
    work.halve(1)
    total = squares(done, 0, sizes[2])
    work.halve(2)
    work.halve(3)
    work.halve(4)
    work.turn()
    work.double(3)
    work.double(2)
    work.double(1)
    work.double(0)
    start(gives[1:2])
    mine = squares(sums, work.mine, work.half)
    work.end()
    start(gives[2:])
    total = total + (mine + squares(sums, work.other, work.half))
    squares_ref[...] = jnp.full(squares_ref.shape, jnp.sum(total))
    wait(gives)


def last_sum(grads, n):
    sizes = [g.shape[0] for g in grads]
    total, mine, unit = sum(sizes), sizes[0] + sizes[1], grads[0].shape[1:]
    out, squares = pl.pallas_call(
        functools.partial(_last_sum, n=n, sizes=sizes),
        in_specs=[ANY] * len(grads),
        out_specs=[ANY, pl.BlockSpec(memory_space=pltpu.VMEM)],
        out_shape=[jax.ShapeDtypeStruct((total, *unit), BF16), jax.ShapeDtypeStruct((8, 128), F32)],
        scratch_shapes=[pltpu.VMEM((k, *unit), BF16) for k in (mine, mine, total - mine, landing(mine))]
        + [pltpu.SemaphoreType.DMA(TALK), pltpu.SemaphoreType.DMA((6,))],
        compiler_params=params(talks=0),
        name="last_sum",
    )(*grads)
    return out.reshape(-1, unit[-1]), squares


def _adamw(squares_ref, *refs, many, count):
    factor = jnp.minimum(1.0, 0.5 * lax.rsqrt(squares_ref[0:1, 0:1] / count + 1e-30))
    for i in range(many):
        w, m, v, g = (refs[4 * i + j][...].astype(F32) for j in range(4))
        g = g * factor
        m = 0.9 * m + 0.1 * g
        v = 0.95 * v + 0.05 * g * g
        w_out, m_out, v_out = refs[4 * many + 3 * i : 4 * many + 3 * i + 3]
        w_out[...] = (w - 0.02 * (m * lax.rsqrt(v + 1e-8) + 0.1 * w)).astype(BF16)
        m_out[...] = m
        v_out[...] = v


def adamw(squares, grads, items, grid, count, name):
    ins, specs, outs, shapes = [squares], [whole(squares.shape)], [], []
    for w, m, v, spec, g_spec in items:
        ins += [w, m, v, grads]
        specs += [spec, spec, spec, g_spec]
        outs += [spec] * 3
        shapes += [jax.ShapeDtypeStruct(x.shape, x.dtype) for x in (w, m, v)]
    size = sum(x[0].size for x in items)
    new = pl.pallas_call(
        functools.partial(_adamw, many=len(items), count=count),
        grid=grid,
        in_specs=specs,
        out_specs=outs,
        out_shape=shapes,
        compiler_params=params(*["arbitrary"] * len(grid)),
        name=name,
    )(*ins)
    return [new[3 * i : 3 * i + 3] for i in range(len(items))]


def optimizer(weights, m, v, grads, squares):
    layers, d, ff = weights[4].shape
    n = ff // d
    pieces = 3 * n + 3
    count = sum(w.size for w in weights)
    rows = fit(d, STEP)
    of_d = d // rows
    wide = pl.BlockSpec((None, rows, d), lambda l, c, r: (l, r, c))
    tall = pl.BlockSpec((None, rows, d), lambda l, c, r: (l, c * of_d + r, 0))
    piece = lambda first: pl.BlockSpec((rows, d), lambda l, c, r: ((l * pieces + first + c) * of_d + r, 0))
    big = adamw(squares, grads, [(weights[i], m[i], v[i], spec, piece(at)) for i, spec, at in ((4, wide, 0), (5, wide, n), (6, tall, n + n))],
                (layers, n, of_d), count, "adamw_mlp")
    nk = weights[1].shape[2]
    row = lambda width: pl.BlockSpec((None, rows // 2, width), lambda l, r: (l, r, 0))
    part = lambda at, width, col: pl.BlockSpec((rows // 2, width), lambda l, r: ((l * pieces + at) * of_d * 2 + r, col))
    small = adamw(squares, grads, [(weights[i], m[i], v[i], row(width), part(pieces - at, width, col)) for i, width, at, col in
                                   ((0, d, 2, 0), (1, nk, 1, 0), (2, nk, 1, 1), (3, d, 3, 0))],
                  (layers, of_d * 2), count, "adamw_attention")
    return small + big


def solution(mesh):
    def step(x, dy, *arrays):
        weights, m, v = (arrays[i * len(NAMES) : (i + 1) * len(NAMES)] for i in range(3))
        wq, wk, wv, wo, wg, wu, wd = weights
        layers = wq.shape[0]
        cos, sin = tables(x.shape[1])
        h, kept = x[0], []
        for n in range(layers):
            q, k, val = project(h, wq, wk, wv, cos, sin, n)
            o, lse = attend(q, k, val)
            last = n == layers - 1
            mid, out = (h, None) if last else mlp(h, o, wo, wg, wu, wd, n)
            kept.append((h, q, k, val, o, lse, mid))
            h = out
        by_h, early, sums, size = dy[0], (), [], mesh.shape["dp"]
        for n in reversed(range(layers)):
            h, q, k, val, o, lse, mid = kept[n]
            group = size if early else 0
            dmid, do, delta, mine, *part = mlp_back(mid, by_h, o, wo, wg, wu, wd, n, n == layers - 1, early, group)
            dq, dk, dv, *done = attend_back(q, k, val, do, lse, delta, *part, units=sum(g.shape[0] for g in early), n=group)
            qkv, *rest = project_back(h, dq, dk, dv, cos, sin, dmid, wq, wk, wv, n, n == 0)
            by_h = rest[0] if rest else None
            sums = done + sums
            early = tuple(g.reshape(-1, UNIT, g.shape[1]) for g in (mine, qkv))
        grads, squares = last_sum([*early, jnp.concatenate(sums) if len(sums) > 1 else sums[0]], size)
        new = optimizer(weights, m, v, grads, squares)
        return tuple(one[which] for which in range(3) for one in new)

    states, all_of = P(("rep", "dp")), P()
    return jax.shard_map(
        step,
        mesh=mesh,
        in_specs=(states, states) + (all_of,) * 21,
        out_specs=(P("rep"),) * 21,
        check_vma=False,
    )
```
